32 devices in a mesh: dp: 4 (over x, y), tp: 8 (over z, core).
Axes of the slice: x: 2, y: 2, z: 4, core: 2. Of those that a mesh axis runs over, the one named last changes fastest.
Arguments:
- x: bfloat16 [8192, 12288], P('dp'), parts along dimension 0
- gain: bfloat16 [12288], replicated
- wq: bfloat16 [12288, 12288], P(None, 'tp')
- wk: bfloat16 [12288, 12288], P(None, 'tp')
- wv: bfloat16 [12288, 12288], P(None, 'tp')
- wo: bfloat16 [12288, 12288], P('tp')
Outputs:
- output: bfloat16 [8192, 12288], P('dp'), parts along dimension 0
There are 4 independent parts. The reference program is written for one: setup_inputs(seed, part) draws one part's arguments, and reference() takes and returns one part's arrays. A program takes and returns all parts, laid end to end along the dimension named above; an argument that names none is the same for every part.
All inputs are finite; a program needn't handle non-finite values.
Results may differ from the reference program's by a relative error of at most 0.012.
Values are sent between devices in bfloat16 or wider.
A program may use at most 2 GiB of HBM per device.

```python
import jax
import jax.numpy as jnp
from jax import lax

ROWS = 2048
D = 12288
HEADS = 96
KV_HEADS = 96
HEAD = 128
THETA = 10000


def setup_inputs(seed: int = 0, part: int = 0) -> dict:
    kx, kn, kq, kk, kv, ko = jax.random.split(jax.random.key(seed), 6)

    def weights(key, rows, columns):
        return jax.random.normal(key, (rows, columns), jnp.float32) * rows**-0.5

    drawn = {
        "x": jax.random.normal(jax.random.fold_in(kx, part), (ROWS, D), jnp.float32),
        "gain": 1 + 0.1 * jax.random.normal(kn, (D,), jnp.float32),
        "wq": 2 * weights(kq, D, HEADS * HEAD),
        "wk": 2 * weights(kk, D, KV_HEADS * HEAD),
        "wv": 4 * weights(kv, D, KV_HEADS * HEAD),
        "wo": weights(ko, HEADS * HEAD, D),
    }
    return {k: v.astype(jnp.bfloat16) for k, v in drawn.items()}


def normed(x, gain):
    wide = x.astype(jnp.float32)
    scale = lax.rsqrt(jnp.mean(wide * wide, -1, keepdims=True) + 1e-6)
    return (wide * scale * gain.astype(jnp.float32)).astype(jnp.bfloat16)


def turned(t, place, theta):
    half = t.shape[-1] // 2
    angle = place.astype(jnp.float32)[:, None] * theta ** (-jnp.arange(half, dtype=jnp.float32) / half)
    cos, sin = jnp.cos(angle)[:, None], jnp.sin(angle)[:, None]
    a, b = t[..., :half].astype(jnp.float32), t[..., half:].astype(jnp.float32)
    return jnp.concatenate([a * cos - b * sin, b * cos + a * sin], -1).astype(jnp.bfloat16)


def matmul(a, w):
    return jnp.dot(a, w, preferred_element_type=jnp.float32).astype(jnp.bfloat16)


def einsum(form, a, b):
    return jnp.einsum(form, a.astype(jnp.float32), b.astype(jnp.float32))


def attention(q, k, v):
    scores = einsum("tgsd,ugd->gstu", q, k) * q.shape[-1] ** -0.5
    token = jnp.arange(q.shape[0])
    scores = jnp.where(token[:, None] >= token, scores, -jnp.inf)
    weights = jax.nn.softmax(scores, -1).astype(jnp.bfloat16)
    return einsum("gstu,ugd->tgsd", weights, v).astype(jnp.bfloat16)


def reference(x, gain, wq, wk, wv, wo):
    a, place = normed(x, gain), jnp.arange(ROWS)
    q = turned(matmul(a, wq).reshape(ROWS, HEADS, HEAD), place, THETA).reshape(ROWS, KV_HEADS, -1, HEAD)
    k = turned(matmul(a, wk).reshape(ROWS, KV_HEADS, HEAD), place, THETA)
    v = matmul(a, wv).reshape(ROWS, KV_HEADS, HEAD)
    seen = attention(q, k, v).reshape(ROWS, HEADS * HEAD)
    return (x.astype(jnp.float32) + jnp.dot(seen, wo, preferred_element_type=jnp.float32)).astype(jnp.bfloat16)
```

```python
import functools

import jax
import jax.numpy as jnp
from jax import lax
from jax.experimental import pallas as pl
from jax.experimental.pallas import tpu as pltpu
from jax.sharding import PartitionSpec as P

HEAD = 128
THETA = 10000
LOG2E = 1.4426950408889634
R = 256
UR, UC = 64, 1536
WT = 256
SLOTS = 3
GROUP = 4
OC = 512
RING = 4
LM = 4
FM, FO, FF = 10, 11, 14
MESH = pl.DeviceIdType.MESH
F32, BF16 = jnp.float32, jnp.bfloat16


def _dot(a, b, ca, cb):
    return lax.dot_general(a, b, (((ca,), (cb,)), ((), ())), preferred_element_type=F32)


def _kernel(x, gain, cos, sin, wq, wk, wv, wo, y, own, part, pin, qin, xn, wb, acc, qb, kb, vb, seen, top, mix, tb, ob, l_own, l_part, l_p,
            l_q, l_x, out, x_s, w_s, tb_s, ob_s, part_s, lo_s, lp_s, lP_s, lq_s, lx_s, out_s, p_s, q_s, y_s, fo_s, fp_s, py_s):
    rows, d = x.shape
    width = wq.shape[1]
    heads, half = width // HEAD, d // 2
    chunks = rows // R
    per = (R // UR) * (half // UC)
    pairs = per * chunks // 2
    tiles = width // WT
    sub = d // width
    n_proj, n_out = 3 * tiles, d // (sub * WT)
    n_tiles = n_proj + n_out

    dp, me = lax.axis_index("dp"), lax.axis_index("tp")
    z, core = me // 2, me % 2
    side = jnp.where(z >= 2, 1, 0)
    mid = (z == 1) | (z == 2)
    end = jnp.logical_not(mid)
    step = 2 - 4 * side
    inner = me + step
    outer = me - step
    partner = me + 1 - 2 * core

    barrier = pltpu.get_barrier_semaphore()
    pl.semaphore_signal(barrier, 1, device_id=(dp, partner), device_id_type=MESH)
    pl.semaphore_signal(barrier, 1, device_id=(dp, inner), device_id_type=MESH)

    @pl.when(mid)
    def _():
        pl.semaphore_signal(barrier, 1, device_id=(dp, outer), device_id_type=MESH)

    pl.semaphore_wait(barrier, jnp.where(mid, 3, 2))


    def start_tile(t, slot):
        for k, w in enumerate((wq, wk, wv)):
            @pl.when((t >= k * tiles) & (t < (k + 1) * tiles))
            def _():
                at = pl.ds(pl.multiple_of((t - k * tiles) * WT, WT), WT)
                pltpu.make_async_copy(w.at[:, at], wb.at[slot], w_s.at[slot]).start()

        @pl.when(t >= n_proj)
        def _():
            for i in range(sub):
                at = lax.rem((t - n_proj) * sub * WT + i * WT + (1 - core) * half, d)
                pltpu.make_async_copy(wo.at[:, pl.ds(pl.multiple_of(at, WT), WT)], wb.at[slot, pl.ds(i * width, width)], w_s.at[slot]).start()

    def wait_tile(slot):
        pltpu.make_async_copy(wq.at[:, pl.ds(0, WT)], wb.at[slot], w_s.at[slot]).wait()

    def next_tile(c, t, slot):
        later = t + SLOTS

        @pl.when((later < n_tiles) | (c < chunks - 1))
        def _():
            start_tile(lax.rem(later, n_tiles), slot)


    def at(unit):
        chunk, i = unit // per, unit % per
        r = chunk * R + (i // (half // UC)) * UR
        u = (i % (half // UC)) * UC
        return pl.ds(pl.multiple_of(r, UR), UR), pl.multiple_of(u, UC)

    def unit_of(p, h):
        return 2 * p + (1 - side if h == 0 else side)

    def region(ref, unit, wide=False):
        r, u = at(unit)
        return ref.at[r, pl.ds(pl.multiple_of(u + core * half, UC) if wide else u, UC)]

    def remote(src, dst, send, recv, to):
        return pltpu.make_async_remote_copy(src_ref=src, dst_ref=dst, send_sem=send, recv_sem=recv, device_id=(dp, to), device_id_type=MESH)

    def loads(p, h):
        unit = unit_of(p, h)
        base = [pltpu.make_async_copy(region(own, unit), l_own.at[h], lo_s.at[h]), pltpu.make_async_copy(region(part, unit), l_part.at[h], lp_s.at[h])]
        in_p = pltpu.make_async_copy(region(pin, unit), l_p.at[h], lP_s.at[h])
        in_q = pltpu.make_async_copy(region(qin, unit), l_q, lq_s)
        in_x = pltpu.make_async_copy(region(x, unit, True), l_x, lx_s)
        return base, in_p, in_q, in_x

    def p_copy(p, h, slot):
        unit = unit_of(p, h)
        return remote(out.at[slot], region(pin, unit), out_s.at[slot, 0], p_s.at[unit], inner)

    def q_copy(p, slot, mine):
        unit = unit_of(p, 1 if mine else 0)
        return remote(out.at[slot], region(qin, unit), out_s.at[slot, 0], q_s.at[p], inner)

    def y_copies(p, slot):
        unit = unit_of(p, 1)
        to = region(y, unit, True)
        return (pltpu.make_async_copy(out.at[slot], to, out_s.at[slot, 0]), remote(out.at[slot], to, out_s.at[slot, 1], y_s.at[unit], inner),
                remote(out.at[slot], to, out_s.at[slot, 2], y_s.at[unit], outer),
                remote(out.at[slot], to, out_s.at[slot, 3], py_s.at[unit // per], partner))

    def sent(p, h):
        slot = (p % 2) * 2 + h
        if h == 0:
            @pl.when(end)
            def _():
                p_copy(p, h, slot).wait_send()

            @pl.when(mid)
            def _():
                q_copy(p, slot, False).wait_send()
        else:
            @pl.when(end)
            def _():
                p_copy(p, h, slot).wait_send()

            @pl.when(mid)
            def _():
                here, *away = y_copies(p, slot)
                here.wait()
                for copy in away:
                    copy.wait_send()

    def load(p, h):
        base, in_p, in_q, in_x = loads(p, h)
        unit = unit_of(p, h)
        if h == 0:
            @pl.when(p % (per // 2) == 0)
            def _():
                c = p // (per // 2)
                whole = part.at[pl.ds(pl.multiple_of(c * R, R), R)]
                pltpu.make_async_copy(whole, whole, part_s.at[c]).wait()

        for copy in base:
            copy.start()

        @pl.when(mid)
        def _():
            remote(out.at[0], region(pin, unit), out_s.at[0, 0], p_s.at[unit], outer).wait_recv()
            in_p.start()
            if h == 1:
                in_x.start()
                q_copy(p, 0, True).wait_recv()
                in_q.start()

    def add(p, h):
        slot = (p % 2) * 2 + h
        base, in_p, in_q, in_x = loads(p, h)

        @pl.when(p >= 2)
        def _():
            sent(p - 2, h)

        for copy in base:
            copy.wait()

        @pl.when(end)
        def _():
            out[slot] = (l_own[h] + l_part[h].astype(F32)).astype(BF16)
            p_copy(p, h, slot).start()

        @pl.when(mid)
        def _():
            in_p.wait()
            if h == 0:
                out[slot] = (l_own[h] + l_part[h].astype(F32) + l_p[h].astype(F32)).astype(BF16)
                q_copy(p, slot, False).start()
            else:
                in_q.wait()
                in_x.wait()
                total = l_own[h] + l_part[h].astype(F32) + l_p[h].astype(F32) + l_q[...].astype(F32)
                out[slot] = (l_x[...].astype(F32) + total).astype(BF16)
                for copy in y_copies(p, slot):
                    copy.start()

    def forward(p, h, on_mid):
        unit = unit_of(p, h)
        here = region(y, unit, True)
        remote(here, here, fp_s.at[0], y_s.at[unit], inner).wait_recv()
        if on_mid:
            remote(here, here, fo_s.at[unit // per], y_s.at[unit], outer).start()
        remote(here, here, fp_s.at[unit // per], py_s.at[unit // per], partner).start()

    def tick(t, h):
        lag = jnp.where(mid, LM, 0)

        def pair(now, k):
            return lax.div(now - lag - k, 2) - jnp.where(mid, k, 0)

        def inside(now, p, k):
            return (now - lag - k >= 0) & (p >= 0) & (p < pairs)

        g = 1 - h
        p1 = pair(t - 1, g)

        @pl.when(inside(t - 1, p1, g))
        def _():
            add(p1, g)

        if h == FM % 2:
            pm = lax.div(t - FM, 2)

            @pl.when(mid & (t >= FM) & (pm < pairs))
            def _():
                forward(pm, 0, True)

        for k, f in ((1, FO), (0, FF)):
            if h == f % 2:
                pe = lax.div(t - f, 2)

                @pl.when(end & (t >= f) & (pe < pairs))
                def _():
                    forward(pe, k, False)

        p0 = pair(t, h)

        @pl.when(inside(t, p0, h))
        def _():
            load(p0, h)

    def ticks(c, t):
        now = per * (c - 1) + lax.div(t, 3) * 2
        for h in range(2):
            @pl.when((c > 0) & (lax.rem(t, 3) == h))
            def _():
                tick(now + h, h)


    def norm(c):
        pltpu.make_async_copy(x.at[pl.ds(0, R)], xn, x_s).wait()

        def some(i, _):
            at = pl.ds(pl.multiple_of(i * 16, 16), 16)
            wide = xn[at, :].astype(F32)
            scale = lax.rsqrt(jnp.mean(wide * wide, -1, keepdims=True) + 1e-6)
            xn[at, :] = (wide * scale * gain[...].astype(F32)).astype(BF16)

        lax.fori_loop(0, R // 16, some, None)

    def project(c):
        here = pl.ds(pl.multiple_of(c * R, R), R)
        hpt = WT // HEAD

        def tile(t, _):
            slot = lax.rem(t, SLOTS)
            wait_tile(slot)
            acc[...] = jnp.dot(xn[...], wb[slot], preferred_element_type=F32)
            next_tile(c, t, slot)
            first = lax.rem(t, tiles) * hpt

            @pl.when(t < 2 * tiles)
            def _():
                for i in range(hpt):
                    wide = acc[:, i * HEAD : (i + 1) * HEAD].astype(BF16).astype(F32)
                    turn = (wide * cos[here, :] + pltpu.roll(wide, HEAD // 2, 1) * sin[here, :]).astype(BF16)

                    @pl.when(t < tiles)
                    def _():
                        qb[first + i] = turn

                    @pl.when(t >= tiles)
                    def _():
                        kb[first + i, here, :] = turn

            @pl.when(t >= 2 * tiles)
            def _():
                for i in range(hpt):
                    vb[first + i, :HEAD, here] = acc[:, i * HEAD : (i + 1) * HEAD].T.astype(BF16)

            ticks(c, t)

        lax.fori_loop(0, n_proj, tile, None)

        @pl.when(c < chunks - 1)
        def _():
            pltpu.make_async_copy(x.at[pl.ds(pl.multiple_of((c + 1) * R, R), R)], xn, x_s).start()

    def attention(c):
        e = HEAD**-0.5 * LOG2E
        visible = lax.broadcasted_iota(jnp.int32, (R, R), 0) <= lax.broadcasted_iota(jnp.int32, (R, R), 1)

        def some(hg, _):
            def block(j, diagonal):
                keys = pl.ds(pl.multiple_of(j * R, R), R)
                scores = [_dot(kb[hg * GROUP + i, keys, :], qb[hg * GROUP + i], 1, 1) for i in range(GROUP)]
                weights, keeps = [], []
                for i, s in enumerate(scores):
                    if diagonal:
                        s = jnp.where(visible, s, -jnp.inf)
                        new = s.max(axis=0, keepdims=True)
                    else:
                        old = top[i]
                        new = jnp.maximum(old, s.max(axis=0, keepdims=True))
                        keeps.append(jnp.exp2((old - new) * e))
                    top[i] = new
                    weights.append(jnp.exp2((s - new) * e).astype(BF16))
                for i, w in enumerate(weights):
                    more = _dot(vb[hg * GROUP + i, :, keys], w, 1, 0)
                    mix[i] = more if diagonal else mix[i] * keeps[i] + more

            block(c, True)
            lax.fori_loop(0, c, lambda j, _: block(j, False), None)
            for i in range(GROUP):
                got = (mix[i, :HEAD, :] * (1 / mix[i, HEAD : HEAD + 1, :])).T.astype(BF16)
                seen[:, pl.ds(pl.multiple_of((hg * GROUP + i) * HEAD, HEAD), HEAD)] = got

        lax.fori_loop(0, heads // GROUP, some, None)

    def project_out(c):
        here = pl.ds(pl.multiple_of(c * R, R), R)
        in_slot = sub * WT // OC
        pieces = half // OC

        def away(i):
            u = pl.ds(pl.multiple_of(i * OC, OC), OC)
            k = lax.rem(i, RING)
            return remote(tb.at[k], part.at[here, u], tb_s.at[k], part_s.at[c], partner)

        def stay(i):
            u = pl.ds(pl.multiple_of(i * OC, OC), OC)
            k = lax.rem(i, RING)
            return pltpu.make_async_copy(ob.at[k], own.at[here, u], ob_s.at[k])

        def tile(t, _, mine):
            slot = lax.rem(t, SLOTS)
            wait_tile(slot)
            first = (t - n_proj) * in_slot - (pieces if mine else 0)

            def piece(i, _):
                n = first + i
                got = [jnp.dot(seen[...], wb[slot, pl.ds(pl.multiple_of((i * (OC // WT) + k) * width, width), width), :], preferred_element_type=F32)
                       for k in range(OC // WT)]
                buf, copy = (ob, stay) if mine else (tb, away)

                @pl.when(n >= RING)
                def _():
                    old = copy(n - RING)
                    old.wait() if mine else old.wait_send()

                for k, g in enumerate(got):
                    buf[lax.rem(n, RING), :, k * WT : (k + 1) * WT] = g.astype(buf.dtype)
                copy(n).start()

            lax.fori_loop(0, in_slot, piece, None)
            next_tile(c, t, slot)
            ticks(c, t)

        lax.fori_loop(n_proj, n_proj + n_out // 2, functools.partial(tile, mine=False), None)
        lax.fori_loop(n_proj + n_out // 2, n_tiles, functools.partial(tile, mine=True), None)
        for i in range(RING):
            away(pieces - RING + i).wait_send()
            stay(pieces - RING + i).wait()

    pltpu.make_async_copy(x.at[pl.ds(0, R)], xn, x_s).start()
    for t in range(SLOTS):
        start_tile(jnp.int32(t), t)
    vb[:, HEAD:, :] = jnp.ones((heads, vb.shape[1] - HEAD, rows), BF16)

    def chunk(c, _):
        norm(c)
        project(c)
        attention(c)
        project_out(c)

    lax.fori_loop(0, chunks, chunk, None)

    first = per * (chunks - 1)
    last = 2 * (pairs - 1) + max(FF, FM, FO, LM + 4) + 1

    def rest(k, _):
        for h in range(2):
            tick(first + 2 * k + h, h)

    lax.fori_loop(0, (last + 1 - first + 1) // 2, rest, None)

    for p in (pairs - 2, pairs - 1):
        for h in range(2):
            sent(p, h)

    def finish(c, _):
        rest_of = y.at[pl.ds(pl.multiple_of(c * R, R), R), pl.ds(pl.multiple_of((1 - core) * half, UC), half)]
        remote(rest_of, rest_of, fp_s.at[c], py_s.at[c], partner).wait_recv()
        few = y.at[pl.ds(0, R), pl.ds(0, half // 2)]

        @pl.when(mid)
        def _():
            remote(few, few, fo_s.at[c], y_s.at[0], outer).wait_send()
            remote(few, few, fp_s.at[c], py_s.at[c], partner).wait_send()

        @pl.when(end)
        def _():
            remote(rest_of, rest_of, fp_s.at[c], py_s.at[c], partner).wait_send()

    lax.fori_loop(0, chunks, finish, None)


def _whole(x, gain, cos, sin, wq, wk, wv, wo):
    rows, d = x.shape
    width = wq.shape[1]
    heads, half = width // HEAD, d // 2
    chunks = rows // R
    units = rows // UR * (half // UC)
    any_space, vmem = pl.BlockSpec(memory_space=pl.ANY), pl.BlockSpec(memory_space=pltpu.VMEM)
    dma = pltpu.SemaphoreType.DMA
    shape = jax.ShapeDtypeStruct
    flops = 2 * rows * d * width * 4 + 2 * rows * rows * width
    return pl.pallas_call(
        _kernel,
        out_shape=[shape((rows, d), BF16), shape((rows, half), F32), shape((rows, half), BF16), shape((rows, half), BF16), shape((rows, half), BF16)],
        in_specs=[any_space, vmem, vmem, vmem, any_space, any_space, any_space, any_space],
        out_specs=[any_space] * 5,
        scratch_shapes=[
            pltpu.VMEM((R, d), BF16),
            pltpu.VMEM((SLOTS, d, WT), BF16),
            pltpu.VMEM((R, WT), F32),
            pltpu.VMEM((heads, R, HEAD), BF16),
            pltpu.VMEM((heads, rows, HEAD), BF16),
            pltpu.VMEM((heads, HEAD + 16, rows), BF16),
            pltpu.VMEM((R, width), BF16),
            pltpu.VMEM((GROUP, 1, R), F32),
            pltpu.VMEM((GROUP, HEAD + 16, R), F32),
            pltpu.VMEM((RING, R, OC), BF16),
            pltpu.VMEM((RING, R, OC), F32),
            pltpu.VMEM((2, UR, UC), F32),
            pltpu.VMEM((2, UR, UC), BF16),
            pltpu.VMEM((2, UR, UC), BF16),
            pltpu.VMEM((UR, UC), BF16),
            pltpu.VMEM((UR, UC), BF16),
            pltpu.VMEM((4, UR, UC), BF16),
            dma, dma((SLOTS,)), dma((RING,)), dma((RING,)),
            dma((chunks,)),
            dma((2,)), dma((2,)), dma((2,)), dma, dma,
            dma((4, 4)),
            dma((units,)), dma((units // 2,)), dma((units,)),
            dma((chunks,)), dma((chunks,)), dma((chunks,)),
        ],
        compiler_params=pltpu.CompilerParams(collective_id=0, has_side_effects=True, vmem_limit_bytes=63 * 2**20),
        cost_estimate=pl.CostEstimate(flops=flops, transcendentals=rows * rows * heads, bytes_accessed=chunks * 4 * d * width * 2),
        name="layer",
    )(x, gain, cos, sin, wq, wk, wv, wo)[0]


def solution(mesh):
    def step(x, gain, wq, wk, wv, wo):
        rows = x.shape[0]
        half = HEAD // 2
        angle = jnp.arange(rows).astype(F32)[:, None] * THETA ** (-jnp.arange(half, dtype=F32) / half)
        cos, sin = jnp.cos(angle), jnp.sin(angle)
        return _whole(x, gain[None], jnp.concatenate([cos, cos], -1), jnp.concatenate([-sin, sin], -1), wq, wk, wv, wo)

    tokens, columns = P("dp", None), P(None, "tp")
    return jax.shard_map(
        step,
        mesh=mesh,
        in_specs=(tokens, P(None), columns, columns, columns, P("tp", None)),
        out_specs=tokens,
        check_vma=False,
    )
```

```python
import functools

import jax
import jax.numpy as jnp
import numpy as np
from jax import lax
from jax.experimental import pallas as pl
from jax.experimental.pallas import tpu as pltpu
from jax.sharding import PartitionSpec as P

HEAD = 128
THETA = 10000
LOG2E = 1.4426950408889634
R = 256
UR, UC = 64, 1536
WT = 256
SLOTS = 3
NR = 16
GROUP = 12
OUT = 4
LM, LB = 4, 1
FM, FO, FF = 10, 11, 14
MESH = pl.DeviceIdType.MESH
F32, BF16 = jnp.float32, jnp.bfloat16


def _dot(a, b, ca, cb):
    return lax.dot_general(a, b, (((ca,), (cb,)), ((), ())), preferred_element_type=F32)


def _kernel(x, gain, cos, sin, wq, wk, wv, wo, y, own, part, pin, qin, xn, wb, acc, qb, kb, vb, seen, top, mix, wide_gain, tb, ob, l_own, l_part, l_p,
            l_q, l_x, out, x_s, w_s, tb_s, ob_s, part_s, lo_s, lp_s, lP_s, lq_s, lx_s, out_s, p_s, q_s, y_s, fo_s, fp_s, py_s):
    rows, d = x.shape
    width = wq.shape[1]
    heads, half = width // HEAD, d // 2
    chunks = rows // R
    per = (R // UR) * (half // UC)
    pairs = per * chunks // 2
    tiles = width // WT
    sub = UC // WT
    n_proj, n_out = 3 * tiles, d // UC
    n_tiles = n_proj + n_out

    dp, me = lax.axis_index("dp"), lax.axis_index("tp")
    z, core = me // 2, me % 2
    side = jnp.where(z >= 2, 1, 0)
    mid = (z == 1) | (z == 2)
    end = jnp.logical_not(mid)
    step = 2 - 4 * side
    inner = me + step
    outer = me - step
    partner = me + 1 - 2 * core

    barrier = pltpu.get_barrier_semaphore()
    pl.semaphore_signal(barrier, 1, device_id=(dp, partner), device_id_type=MESH)
    pl.semaphore_signal(barrier, 1, device_id=(dp, inner), device_id_type=MESH)

    @pl.when(mid)
    def _():
        pl.semaphore_signal(barrier, 1, device_id=(dp, outer), device_id_type=MESH)

    pl.semaphore_wait(barrier, jnp.where(mid, 3, 2))


    def start_tile(t, slot):
        for k, w in enumerate((wq, wk, wv)):
            @pl.when((t >= k * tiles) & (t < (k + 1) * tiles))
            def _():
                at = pl.ds(pl.multiple_of((t - k * tiles) * WT, WT), WT)
                pltpu.make_async_copy(w.at[:, at], wb.at[slot], w_s.at[slot]).start()

        @pl.when(t >= n_proj)
        def _():
            for i in range(sub):
                k = t - n_proj
                at = lax.rem(k + 1 - core, 2) * half + lax.div(k, 2) * UC + i * WT
                pltpu.make_async_copy(wo.at[:, pl.ds(pl.multiple_of(at, WT), WT)], wb.at[slot, pl.ds(i * width, width)], w_s.at[slot]).start()

    def wait_tile(slot, n):
        some = wb.at[slot, pl.ds(0, n)]
        pltpu.make_async_copy(some, some, w_s.at[slot]).wait()

    def next_tile(c, t, slot):
        later = t + SLOTS

        @pl.when((later < n_tiles) | (c < chunks - 1))
        def _():
            start_tile(lax.rem(later, n_tiles), slot)


    def at(unit):
        chunk, i = lax.div(unit, per), lax.rem(unit, per)
        r = chunk * R + lax.rem(i, R // UR) * UR
        u = lax.div(i, R // UR) * UC
        return pl.ds(pl.multiple_of(r, UR), UR), pl.multiple_of(u, UC)

    def unit_of(p, h):
        return 2 * p + (1 - side if h == 0 else side)

    def region(ref, unit, wide=False):
        r, u = at(unit)
        return ref.at[r, pl.ds(pl.multiple_of(u + core * half, UC) if wide else u, UC)]

    def remote(src, dst, send, recv, to):
        return pltpu.make_async_remote_copy(src_ref=src, dst_ref=dst, send_sem=send, recv_sem=recv, device_id=(dp, to), device_id_type=MESH)

    def loads(p, h):
        unit = unit_of(p, h)
        base = (lambda: pltpu.make_async_copy(region(own, unit), l_own.at[h], lo_s.at[h]),
                lambda: pltpu.make_async_copy(region(part, unit), l_part.at[h], lp_s.at[h]))
        in_p = lambda: pltpu.make_async_copy(region(pin, unit), l_p.at[h], lP_s.at[h])
        in_q = lambda: pltpu.make_async_copy(region(qin, unit), l_q, lq_s)
        in_x = lambda: pltpu.make_async_copy(region(x, unit, True), l_x, lx_s)
        return base, in_p, in_q, in_x

    def p_copy(p, h, slot):
        unit = unit_of(p, h)
        return remote(out.at[slot], region(pin, unit), out_s.at[slot, 0], p_s.at[unit], inner)

    def q_copy(p, slot, mine):
        unit = unit_of(p, 1 if mine else 0)
        return remote(out.at[slot], region(qin, unit), out_s.at[slot, 0], q_s.at[p], inner)

    def y_copies(p, slot):
        unit = unit_of(p, 1)
        to = region(y, unit, True)
        return (pltpu.make_async_copy(out.at[slot], to, out_s.at[slot, 0]), remote(out.at[slot], to, out_s.at[slot, 1], y_s.at[unit], inner),
                remote(out.at[slot], to, out_s.at[slot, 2], y_s.at[unit], outer),
                remote(out.at[slot], to, out_s.at[slot, 3], py_s.at[lax.div(unit, per)], partner))

    def sent(p, h):
        slot = lax.rem(p, OUT // 2) * 2 + h
        if h == 0:
            @pl.when(end)
            def _():
                p_copy(p, h, slot).wait_send()

            @pl.when(mid)
            def _():
                q_copy(p, slot, False).wait_send()
        else:
            @pl.when(end)
            def _():
                p_copy(p, h, slot).wait_send()

            @pl.when(mid)
            def _():
                here, *away = y_copies(p, slot)
                here.wait()
                for copy in away:
                    copy.wait_send()

    def load(p, h):
        base, in_p, in_q, in_x = loads(p, h)
        unit = unit_of(p, h)
        if h == 0:
            @pl.when(lax.rem(p, R // UR // 2) == 0)
            def _():
                whole = part.at[pl.ds(0, R), pl.ds(0, UC)]
                pltpu.make_async_copy(whole, whole, part_s.at[lax.div(p, R // UR // 2)]).wait()

        for copy in base:
            copy().start()

        @pl.when(mid)
        def _():
            remote(out.at[0], region(pin, unit), out_s.at[0, 0], p_s.at[unit], outer).wait_recv()
            in_p().start()
            if h == 1:
                in_x().start()
                q_copy(p, 0, True).wait_recv()
                in_q().start()

    def add(p, h):
        slot = lax.rem(p, OUT // 2) * 2 + h
        base, in_p, in_q, in_x = loads(p, h)

        @pl.when(p >= OUT // 2)
        def _():
            sent(p - OUT // 2, h)

        for copy in base:
            copy().wait()

        @pl.when(end)
        def _():
            out[slot] = (l_own[h] + l_part[h].astype(F32)).astype(BF16)
            p_copy(p, h, slot).start()

        @pl.when(mid)
        def _():
            in_p().wait()
            if h == 0:
                out[slot] = (l_own[h] + l_part[h].astype(F32) + l_p[h].astype(F32)).astype(BF16)
                q_copy(p, slot, False).start()
            else:
                in_q().wait()
                in_x().wait()
                total = l_own[h] + l_part[h].astype(F32) + l_p[h].astype(F32) + l_q[...].astype(F32)
                out[slot] = (l_x[...].astype(F32) + total).astype(BF16)
                for copy in y_copies(p, slot):
                    copy.start()

    def forward(p, h, on_mid):
        unit = unit_of(p, h)
        here = region(y, unit, True)
        remote(here, here, fp_s.at[0], y_s.at[unit], inner).wait_recv()
        if on_mid:
            remote(here, here, fo_s.at[lax.div(unit, per)], y_s.at[unit], outer).start()
        remote(here, here, fp_s.at[lax.div(unit, per)], py_s.at[lax.div(unit, per)], partner).start()

    def tick(t, h):
        lag = jnp.where(mid, LM, 0)

        def pair(now, k):
            return lax.div(now - lag - k, 2) - jnp.where(mid, LB * k, 0)

        def inside(now, p, k):
            return (now - lag - k >= 0) & (p >= 0) & (p < pairs)

        g = 1 - h
        p1 = pair(t - 1, g)

        @pl.when(inside(t - 1, p1, g))
        def _():
            add(p1, g)

        if h == FM % 2:
            pm = lax.div(t - FM, 2)

            @pl.when(mid & (t >= FM) & (pm < pairs))
            def _():
                forward(pm, 0, True)

        for k, f in ((1, FO), (0, FF)):
            if h == f % 2:
                pe = lax.div(t - f, 2)

                @pl.when(end & (t >= f) & (pe < pairs))
                def _():
                    forward(pe, k, False)

        p0 = pair(t, h)

        @pl.when(inside(t, p0, h))
        def _():
            load(p0, h)

    late = per // (half // UC)
    n_early = n_proj + 4

    def ticks(c, at):
        early = at < n_early
        a = jnp.where(early, lax.div(at * (per - late), n_early), lax.div((at - n_early) * late, n_tiles + 2 - n_early))
        b = jnp.where(early, lax.div((at + 1) * (per - late), n_early), lax.div((at + 1 - n_early) * late, n_tiles + 2 - n_early))
        now = jnp.where(early, per * (c - 1) + late, per * c) + a
        for h in range(2):
            @pl.when((now >= 0) & (b > a) & (lax.rem(now, 2) == h))
            def _():
                tick(now, h)


    def norm(i):
        at = pl.ds(pl.multiple_of(i * NR, NR), NR)
        wide = xn[at, :].astype(F32)
        scale = lax.rsqrt(jnp.mean(wide * wide, -1, keepdims=True) + 1e-6)
        xn[at, :] = (wide * scale * jnp.concatenate([wide_gain[...]] * (NR // 8), 0)).astype(BF16)

    def wait_x():
        pltpu.make_async_copy(x.at[pl.ds(0, R)], xn, x_s).wait()

    def project(c):
        here = pl.ds(pl.multiple_of(c * R, R), R)
        hpt = WT // HEAD

        def tile(t, _):
            slot = lax.rem(c * n_tiles + t, SLOTS)
            wait_tile(slot, d)
            acc[...] = jnp.dot(xn[...], wb[slot], preferred_element_type=F32)
            next_tile(c, t, slot)
            first = lax.rem(t, tiles) * hpt

            @pl.when(t < 2 * tiles)
            def _():
                for i in range(hpt):
                    wide = acc[:, i * HEAD : (i + 1) * HEAD].astype(BF16).astype(F32)
                    turn = (wide * cos[here, :] + pltpu.roll(wide, HEAD // 2, 1) * sin[here, :]).astype(BF16)

                    @pl.when(t < tiles)
                    def _():
                        qb[first + i] = turn

                    @pl.when(t >= tiles)
                    def _():
                        kb[first + i, here, :] = turn

            @pl.when(t >= 2 * tiles)
            def _():
                for i in range(hpt):
                    vb[first + i, :HEAD, here] = acc[:, i * HEAD : (i + 1) * HEAD].T.astype(BF16)

            ticks(c, t + 1)

        lax.fori_loop(0, n_proj, tile, None)

        @pl.when(c < chunks - 1)
        def _():
            pltpu.make_async_copy(x.at[pl.ds(pl.multiple_of((c + 1) * R, R), R)], xn, x_s).start()

    def attention(c):
        e = HEAD**-0.5 * LOG2E

        def some(hg, _):
            def block(start, n, diagonal):
                keys = pl.ds(pl.multiple_of(start, R), n)
                scores = [_dot(kb[hg * GROUP + i, keys, :], qb[hg * GROUP + i], 1, 1) for i in range(GROUP)]
                if diagonal:
                    visible = lax.broadcasted_iota(jnp.int32, (n, R), 0) - (n - R) <= lax.broadcasted_iota(jnp.int32, (n, R), 1)
                weights, keeps = [], []
                for i, s in enumerate(scores):
                    if diagonal:
                        s = jnp.where(visible, s, -jnp.inf)
                        new = s.max(axis=0, keepdims=True)
                    else:
                        old = top[i]
                        new = jnp.maximum(old, s.max(axis=0, keepdims=True))
                        keeps.append(jnp.exp2((old - new) * e))
                    top[i] = new
                    weights.append(jnp.exp2((s - new) * e).astype(BF16))
                for i, w in enumerate(weights):
                    more = _dot(vb[hg * GROUP + i, :, keys], w, 1, 0)
                    mix[i] = more if diagonal else mix[i] * keeps[i] + more

            odd = lax.rem(c, 2)

            @pl.when(odd == 0)
            def _():
                block(c * R, R, True)

            @pl.when(odd == 1)
            def _():
                block((c - 1) * R, 2 * R, True)

            lax.fori_loop(0, lax.div(c, 2), lambda j, _: block(j * 2 * R, 2 * R, False), None)
            for i in range(GROUP):
                got = (mix[i, :HEAD, :] * (1 / mix[i, HEAD : HEAD + 1, :])).T.astype(BF16)
                seen[:, pl.ds(pl.multiple_of((hg * GROUP + i) * HEAD, HEAD), HEAD)] = got

        lax.fori_loop(0, heads // GROUP, some, None)

    def away(c, u):
        here = part.at[pl.ds(pl.multiple_of(c * R, R), R), pl.ds(pl.multiple_of(u * UC, UC), UC)]
        return remote(tb.at[lax.rem(u, 2)], here, tb_s.at[lax.rem(u, 2)], part_s.at[c * (half // UC) + u], partner)

    def stay(c, u):
        return pltpu.make_async_copy(ob, own.at[pl.ds(pl.multiple_of(c * R, R), R), pl.ds(pl.multiple_of(u * UC, UC), UC)], ob_s)

    def project_out(c):
        def dots(t):
            slot = lax.rem(c * n_tiles + t, SLOTS)
            wait_tile(slot, sub * width)
            for k in range(sub):
                yield slice(k * WT, (k + 1) * WT), jnp.dot(seen[...], wb[slot, k * width : (k + 1) * width, :], preferred_element_type=F32)
            next_tile(c, t, slot)

        def columns(u, _):
            t = n_proj + 2 * u

            @pl.when((c > 0) | (u >= 2))
            def _():
                away(c, u).wait_send()

            for at, got in dots(t):
                tb[lax.rem(u, 2), :, at] = got.astype(BF16)
            away(c, u).start()

            @pl.when(u > 0)
            def _():
                stay(c, u - 1).wait()

            ticks(c, t + 2)
            for at, got in dots(t + 1):
                ob[:, at] = got
            stay(c, u).start()
            ticks(c, t + 3)

        lax.fori_loop(0, half // UC, columns, None)

    pltpu.make_async_copy(x.at[pl.ds(0, R)], xn, x_s).start()
    for t in range(SLOTS):
        start_tile(jnp.int32(t), t)
    vb[:, HEAD:, :] = jnp.ones((heads, vb.shape[1] - HEAD, rows), BF16)

    wide_gain[...] = jnp.broadcast_to(gain[...].astype(F32), wide_gain.shape)

    def chunk(c, _):
        wait_x()
        lax.fori_loop(0, R // NR, lambda i, _: norm(i), None)

        @pl.when(c > 0)
        def _():
            stay(c, 0).wait()

        ticks(c, jnp.int32(0))
        project(c)
        attention(c)
        ticks(c, jnp.int32(n_proj + 1))
        project_out(c)

    lax.fori_loop(0, chunks, chunk, None)

    stay(0, 0).wait()
    for u in range(2):
        away(0, u).wait_send()
    first = per * (chunks - 1) + late
    last = 2 * (pairs - 1) + max(FF, FM, FO, LM + 2 * LB + 2) + 1

    def rest(k, _):
        for h in range(2):
            tick(first + 2 * k + h, h)

    lax.fori_loop(0, (last + 1 - first + 1) // 2, rest, None)

    for p in range(pairs - OUT // 2, pairs):
        for h in range(2):
            sent(jnp.int32(p), h)

    def finish(c, _):
        rest_of = y.at[pl.ds(pl.multiple_of(c * R, R), R), pl.ds(pl.multiple_of((1 - core) * half, UC), half)]
        remote(rest_of, rest_of, fp_s.at[c], py_s.at[c], partner).wait_recv()
        few = y.at[pl.ds(0, R), pl.ds(0, half // 2)]

        @pl.when(mid)
        def _():
            remote(few, few, fo_s.at[c], y_s.at[0], outer).wait_send()
            remote(few, few, fp_s.at[c], py_s.at[c], partner).wait_send()

        @pl.when(end)
        def _():
            remote(rest_of, rest_of, fp_s.at[c], py_s.at[c], partner).wait_send()

    lax.fori_loop(0, chunks, finish, None)


def _whole(x, gain, cos, sin, wq, wk, wv, wo):
    rows, d = x.shape
    width = wq.shape[1]
    heads, half = width // HEAD, d // 2
    chunks = rows // R
    units = rows // UR * (half // UC)
    any_space, vmem = pl.BlockSpec(memory_space=pl.ANY), pl.BlockSpec(memory_space=pltpu.VMEM)
    dma = pltpu.SemaphoreType.DMA
    shape = jax.ShapeDtypeStruct
    flops = 2 * rows * d * width * 4 + 2 * rows * rows * width
    return pl.pallas_call(
        _kernel,
        out_shape=[shape((rows, d), BF16), shape((rows, half), F32), shape((rows, half), BF16), shape((rows, half), BF16), shape((rows, half), BF16)],
        in_specs=[any_space, vmem, vmem, vmem, any_space, any_space, any_space, any_space],
        out_specs=[any_space] * 5,
        scratch_shapes=[
            pltpu.VMEM((R, d), BF16),
            pltpu.VMEM((SLOTS, d, WT), BF16),
            pltpu.VMEM((R, WT), F32),
            pltpu.VMEM((heads, R, HEAD), BF16),
            pltpu.VMEM((heads, rows, HEAD), BF16),
            pltpu.VMEM((heads, HEAD + 16, rows), BF16),
            pltpu.VMEM((R, width), BF16),
            pltpu.VMEM((GROUP, 1, R), F32),
            pltpu.VMEM((GROUP, HEAD + 16, R), F32),
            pltpu.VMEM((8, d), F32),
            pltpu.VMEM((2, R, UC), BF16),
            pltpu.VMEM((R, UC), F32),
            pltpu.VMEM((2, UR, UC), F32),
            pltpu.VMEM((2, UR, UC), BF16),
            pltpu.VMEM((2, UR, UC), BF16),
            pltpu.VMEM((UR, UC), BF16),
            pltpu.VMEM((UR, UC), BF16),
            pltpu.VMEM((OUT, UR, UC), BF16),
            dma, dma((SLOTS,)), dma((2,)), dma,
            dma((chunks * (half // UC),)),
            dma((2,)), dma((2,)), dma((2,)), dma, dma,
            dma((OUT, 4)),
            dma((units,)), dma((units // 2,)), dma((units,)),
            dma((chunks,)), dma((chunks,)), dma((chunks,)),
        ],
        compiler_params=pltpu.CompilerParams(collective_id=0, has_side_effects=True, vmem_limit_bytes=63 * 2**20),
        cost_estimate=pl.CostEstimate(flops=flops, transcendentals=rows * rows * heads, bytes_accessed=chunks * 4 * d * width * 2),
        name="layer",
    )(x, gain, cos, sin, wq, wk, wv, wo)[0]


def _turns(rows):
    half = HEAD // 2
    angle = np.arange(rows, dtype=np.float32)[:, None] * (float(THETA) ** (-np.arange(half) / half)).astype(np.float32)
    cos, sin = (f(angle.astype(np.float64)).astype(np.float32) for f in (np.cos, np.sin))
    return np.concatenate([cos, cos], -1), np.concatenate([-sin, sin], -1)


def solution(mesh):
    def step(x, gain, wq, wk, wv, wo):
        cos, sin = _turns(x.shape[0])
        return _whole(x, gain[None], jnp.asarray(cos), jnp.asarray(sin), wq, wk, wv, wo)

    tokens, columns = P("dp", None), P(None, "tp")
    return jax.shard_map(
        step,
        mesh=mesh,
        in_specs=(tokens, P(None), columns, columns, columns, P("tp", None)),
        out_specs=tokens,
        check_vma=False,
    )
```

```python
import functools

import jax
import jax.numpy as jnp
import numpy as np
from jax import lax
from jax.experimental import pallas as pl
from jax.experimental.pallas import tpu as pltpu
from jax.sharding import PartitionSpec as P

HEAD = 128
THETA = 10000
LOG2E = 1.4426950408889634
R = 256
UR, UC = 64, 1536
WT = 256
SLOTS = 3
NR = 32
GROUP = 6
OUT = 4
LM, LB = 4, 1
FM, FO, FF = 10, 11, 14
MESH = pl.DeviceIdType.MESH
F32, BF16 = jnp.float32, jnp.bfloat16


def _dot(a, b, ca, cb):
    return lax.dot_general(a, b, (((ca,), (cb,)), ((), ())), preferred_element_type=F32)


def _kernel(x, gain, cos, sin, wq, wk, wv, wo, y, own, part, pin, qin, xn, wb, acc, qb, kb, vb, seen, top, mix, wide_gain, tb, ob, l_own, l_part, l_p,
            l_q, l_x, out, x_s, w_s, tb_s, ob_s, part_s, lo_s, lp_s, lP_s, lq_s, lx_s, xs_s, xr_s, free_s, out_s, p_s, q_s, y_s, fo_s, fp_s, py_s):
    rows, d = x.shape
    width = wq.shape[1]
    heads, half = width // HEAD, d // 2
    chunks = rows // R
    per = (R // UR) * (half // UC)
    pairs = per * chunks // 2
    tiles = width // WT
    sub = UC // WT
    n_proj, n_out = 3 * tiles, d // UC
    n_tiles = n_proj + n_out

    dp, me = lax.axis_index("dp"), lax.axis_index("tp")
    z, core = me // 2, me % 2
    side = jnp.where(z >= 2, 1, 0)
    mid = (z == 1) | (z == 2)
    end = jnp.logical_not(mid)
    step = 2 - 4 * side
    inner = me + step
    outer = me - step
    partner = me + 1 - 2 * core

    barrier = pltpu.get_barrier_semaphore()
    pl.semaphore_signal(barrier, 1, device_id=(dp, partner), device_id_type=MESH)
    pl.semaphore_signal(barrier, 1, device_id=(dp, inner), device_id_type=MESH)

    @pl.when(mid)
    def _():
        pl.semaphore_signal(barrier, 1, device_id=(dp, outer), device_id_type=MESH)

    pl.semaphore_wait(barrier, jnp.where(mid, 3, 2))


    def start_tile(t, slot):
        for k, w in enumerate((wq, wk, wv)):
            @pl.when((t >= k * tiles) & (t < (k + 1) * tiles))
            def _():
                at = pl.ds(pl.multiple_of((t - k * tiles) * WT, WT), WT)
                pltpu.make_async_copy(w.at[:, at], wb.at[slot], w_s.at[slot]).start()

        @pl.when(t >= n_proj)
        def _():
            for i in range(sub):
                k = t - n_proj
                at = lax.rem(k + 1 - core, 2) * half + lax.div(k, 2) * UC + i * WT
                pltpu.make_async_copy(wo.at[:, pl.ds(pl.multiple_of(at, WT), WT)], wb.at[slot, pl.ds(i * width, width)], w_s.at[slot]).start()

    def wait_tile(slot, n):
        some = wb.at[slot, pl.ds(0, n)]
        pltpu.make_async_copy(some, some, w_s.at[slot]).wait()

    def next_tile(c, t, slot):
        later = t + SLOTS

        @pl.when((later < n_tiles) | (c < chunks - 1))
        def _():
            start_tile(lax.rem(later, n_tiles), slot)


    def at(unit):
        chunk, i = lax.div(unit, per), lax.rem(unit, per)
        r = chunk * R + lax.rem(i, R // UR) * UR
        u = lax.div(i, R // UR) * UC
        return pl.ds(pl.multiple_of(r, UR), UR), pl.multiple_of(u, UC)

    def unit_of(p, h):
        return 2 * p + (1 - side if h == 0 else side)

    def region(ref, unit, wide=False):
        r, u = at(unit)
        return ref.at[r, pl.ds(pl.multiple_of(u + core * half, UC) if wide else u, UC)]

    def remote(src, dst, send, recv, to):
        return pltpu.make_async_remote_copy(src_ref=src, dst_ref=dst, send_sem=send, recv_sem=recv, device_id=(dp, to), device_id_type=MESH)

    def loads(p, h):
        unit = unit_of(p, h)
        base = (lambda: pltpu.make_async_copy(region(own, unit), l_own.at[h], lo_s.at[h]),
                lambda: pltpu.make_async_copy(region(part, unit), l_part.at[h], lp_s.at[h]))
        in_p = lambda: pltpu.make_async_copy(region(pin, unit), l_p.at[h], lP_s.at[h])
        in_q = lambda: pltpu.make_async_copy(region(qin, unit), l_q, lq_s)
        in_x = lambda: pltpu.make_async_copy(region(x, unit, True), l_x, lx_s)
        return base, in_p, in_q, in_x

    def p_copy(p, h, slot):
        unit = unit_of(p, h)
        return remote(out.at[slot], region(pin, unit), out_s.at[slot, 0], p_s.at[unit], inner)

    def q_copy(p, slot, mine):
        unit = unit_of(p, 1 if mine else 0)
        return remote(out.at[slot], region(qin, unit), out_s.at[slot, 0], q_s.at[p], inner)

    def y_copies(p, slot):
        unit = unit_of(p, 1)
        to = region(y, unit, True)
        return (pltpu.make_async_copy(out.at[slot], to, out_s.at[slot, 0]), remote(out.at[slot], to, out_s.at[slot, 1], y_s.at[unit], inner),
                remote(out.at[slot], to, out_s.at[slot, 2], y_s.at[unit], outer),
                remote(out.at[slot], to, out_s.at[slot, 3], py_s.at[lax.div(unit, per)], partner))

    def sent(p, h):
        slot = lax.rem(p, OUT // 2) * 2 + h
        if h == 0:
            @pl.when(end)
            def _():
                p_copy(p, h, slot).wait_send()

            @pl.when(mid)
            def _():
                q_copy(p, slot, False).wait_send()
        else:
            @pl.when(end)
            def _():
                p_copy(p, h, slot).wait_send()

            @pl.when(mid)
            def _():
                here, *away = y_copies(p, slot)
                here.wait()
                for copy in away:
                    copy.wait_send()

    def load(p, h):
        base, in_p, in_q, in_x = loads(p, h)
        unit = unit_of(p, h)
        if h == 0:
            @pl.when(lax.rem(p, R // UR // 2) == 0)
            def _():
                whole = part.at[pl.ds(0, R), pl.ds(0, UC)]
                pltpu.make_async_copy(whole, whole, part_s.at[lax.div(p, R // UR // 2)]).wait()

        for copy in base:
            copy().start()

        @pl.when(mid)
        def _():
            remote(out.at[0], region(pin, unit), out_s.at[0, 0], p_s.at[unit], outer).wait_recv()
            in_p().start()
            if h == 1:
                in_x().start()
                q_copy(p, 0, True).wait_recv()
                in_q().start()

    def add(p, h):
        slot = lax.rem(p, OUT // 2) * 2 + h
        base, in_p, in_q, in_x = loads(p, h)

        @pl.when(p >= OUT // 2)
        def _():
            sent(p - OUT // 2, h)

        for copy in base:
            copy().wait()

        @pl.when(end)
        def _():
            out[slot] = (l_own[h] + l_part[h].astype(F32)).astype(BF16)
            p_copy(p, h, slot).start()

        @pl.when(mid)
        def _():
            in_p().wait()
            if h == 0:
                out[slot] = (l_own[h] + l_part[h].astype(F32) + l_p[h].astype(F32)).astype(BF16)
                q_copy(p, slot, False).start()
            else:
                in_q().wait()
                in_x().wait()
                total = l_own[h] + l_part[h].astype(F32) + l_p[h].astype(F32) + l_q[...].astype(F32)
                out[slot] = (l_x[...].astype(F32) + total).astype(BF16)
                for copy in y_copies(p, slot):
                    copy.start()

    def forward(p, h, on_mid):
        unit = unit_of(p, h)
        here = region(y, unit, True)
        remote(here, here, fp_s.at[0], y_s.at[unit], inner).wait_recv()
        if on_mid:
            remote(here, here, fo_s.at[lax.div(unit, per)], y_s.at[unit], outer).start()
        remote(here, here, fp_s.at[lax.div(unit, per)], py_s.at[lax.div(unit, per)], partner).start()

    def tick(t, h):
        lag = jnp.where(mid, LM, 0)

        def pair(now, k):
            return lax.div(now - lag - k, 2) - jnp.where(mid, LB * k, 0)

        def inside(now, p, k):
            return (now - lag - k >= 0) & (p >= 0) & (p < pairs)

        g = 1 - h
        p1 = pair(t - 1, g)

        @pl.when(inside(t - 1, p1, g))
        def _():
            add(p1, g)

        if h == FM % 2:
            pm = lax.div(t - FM, 2)

            @pl.when(mid & (t >= FM) & (pm < pairs))
            def _():
                forward(pm, 0, True)

        for k, f in ((1, FO), (0, FF)):
            if h == f % 2:
                pe = lax.div(t - f, 2)

                @pl.when(end & (t >= f) & (pe < pairs))
                def _():
                    forward(pe, k, False)

        p0 = pair(t, h)

        @pl.when(inside(t, p0, h))
        def _():
            load(p0, h)

    late = per // (half // UC)
    n_points = 1 + n_tiles + heads // GROUP
    n_early = n_points - (n_out - 2)

    def ticks(c, at):
        early = at < n_early
        some = n_points - n_early
        a = jnp.where(early, lax.div(at * (per - late) + n_early - 1, n_early), lax.div((at - n_early) * late + some - 1, some))
        b = jnp.where(early, lax.div((at + 1) * (per - late) + n_early - 1, n_early), lax.div((at + 1 - n_early) * late + some - 1, some))
        now = jnp.where(early, per * (c - 1) + late, per * c) + a
        for h in range(2):
            @pl.when((now >= 0) & (b > a) & (lax.rem(now, 2) == h))
            def _():
                tick(now, h)


    def norm(i):
        at = pl.ds(pl.multiple_of(i * NR, NR), NR)
        wide = xn[at, :].astype(F32)
        scale = lax.rsqrt(jnp.mean(wide * wide, -1, keepdims=True) + 1e-6)
        xn[at, :] = (wide * scale * jnp.concatenate([wide_gain[...]] * (NR // 8), 0)).astype(BF16)

    mine = pl.ds(pl.multiple_of(core * (R // 2), R // 2), R // 2)

    def take_x(c):
        return pltpu.make_async_copy(x.at[pl.ds(pl.multiple_of(c * R + core * (R // 2), R // 2), R // 2)], xn.at[mine], x_s)

    def share():
        return remote(xn.at[mine], xn.at[mine], xs_s, xr_s, partner)

    def next_norm(c):
        take_x(c + 1).wait()
        lax.fori_loop(0, R // 2 // NR, lambda i, _: norm(core * (R // 2 // NR) + i), None)
        pl.semaphore_wait(free_s, 1)
        share().start()

    def project(c):
        here = pl.ds(pl.multiple_of(c * R, R), R)
        hpt = WT // HEAD

        def tile(t, _):
            slot = lax.rem(c * n_tiles + t, SLOTS)
            wait_tile(slot, d)
            acc[...] = jnp.dot(xn[...], wb[slot], preferred_element_type=F32)
            next_tile(c, t, slot)
            first = lax.rem(t, tiles) * hpt

            @pl.when(t < 2 * tiles)
            def _():
                for i in range(hpt):
                    wide = acc[:, i * HEAD : (i + 1) * HEAD].astype(BF16).astype(F32)
                    turn = (wide * cos[here, :] + pltpu.roll(wide, HEAD // 2, 1) * sin[here, :]).astype(BF16)

                    @pl.when(t < tiles)
                    def _():
                        qb[first + i] = turn

                    @pl.when(t >= tiles)
                    def _():
                        kb[first + i, here, :] = turn

            @pl.when(t >= 2 * tiles)
            def _():
                for i in range(hpt):
                    vb[first + i, :HEAD, here] = acc[:, i * HEAD : (i + 1) * HEAD].T.astype(BF16)

            ticks(c, t + 1)

        lax.fori_loop(0, n_proj, tile, None)

        @pl.when(c < chunks - 1)
        def _():
            pl.semaphore_signal(free_s, 1, device_id=(dp, partner), device_id_type=MESH)
            take_x(c + 1).start()

    def attention(c):
        e = HEAD**-0.5 * LOG2E

        def some(hg, _):
            def block(start, n, diagonal):
                keys = pl.ds(pl.multiple_of(start, R), n)
                scores = [_dot(kb[hg * GROUP + i, keys, :], qb[hg * GROUP + i], 1, 1) for i in range(GROUP)]
                if diagonal:
                    visible = lax.broadcasted_iota(jnp.int32, (n, R), 0) - (n - R) <= lax.broadcasted_iota(jnp.int32, (n, R), 1)
                weights, keeps = [], []
                for i, s in enumerate(scores):
                    if diagonal:
                        s = jnp.where(visible, s, -jnp.inf)
                        new = s.max(axis=0, keepdims=True)
                    else:
                        old = top[i]
                        new = jnp.maximum(old, s.max(axis=0, keepdims=True))
                        keeps.append(jnp.exp2((old - new) * e))
                    top[i] = new
                    weights.append(jnp.exp2((s - new) * e).astype(BF16))
                for i, w in enumerate(weights):
                    more = _dot(vb[hg * GROUP + i, :, keys], w, 1, 0)
                    mix[i] = more if diagonal else mix[i] * keeps[i] + more

            odd = lax.rem(c, 2)

            @pl.when(odd == 0)
            def _():
                block(c * R, R, True)

            @pl.when(odd == 1)
            def _():
                block((c - 1) * R, 2 * R, True)

            lax.fori_loop(0, lax.div(c, 2), lambda j, _: block(j * 2 * R, 2 * R, False), None)
            for i in range(GROUP):
                got = (mix[i, :HEAD, :] * (1 / mix[i, HEAD : HEAD + 1, :])).T.astype(BF16)
                seen[:, pl.ds(pl.multiple_of((hg * GROUP + i) * HEAD, HEAD), HEAD)] = got

            ticks(c, n_proj + 1 + hg)

        lax.fori_loop(0, heads // GROUP, some, None)

    def away(c, u):
        here = part.at[pl.ds(pl.multiple_of(c * R, R), R), pl.ds(pl.multiple_of(u * UC, UC), UC)]
        return remote(tb.at[lax.rem(u, 2)], here, tb_s.at[lax.rem(u, 2)], part_s.at[c * (half // UC) + u], partner)

    def stay(c, u):
        return pltpu.make_async_copy(ob, own.at[pl.ds(pl.multiple_of(c * R, R), R), pl.ds(pl.multiple_of(u * UC, UC), UC)], ob_s)

    def project_out(c):
        def dots(t):
            slot = lax.rem(c * n_tiles + t, SLOTS)
            wait_tile(slot, sub * width)
            for k in range(sub):
                yield slice(k * WT, (k + 1) * WT), jnp.dot(seen[...], wb[slot, k * width : (k + 1) * width, :], preferred_element_type=F32)
            next_tile(c, t, slot)

        def columns(u, _):
            t = n_proj + 2 * u

            @pl.when((c > 0) | (u >= 2))
            def _():
                away(c, u).wait_send()

            for at, got in dots(t):
                tb[lax.rem(u, 2), :, at] = got.astype(BF16)
            away(c, u).start()

            @pl.when(u > 0)
            def _():
                stay(c, u - 1).wait()

            ticks(c, t + 1 + heads // GROUP)

            @pl.when((u == 1) & (c < chunks - 1))
            def _():
                next_norm(c)

            for at, got in dots(t + 1):
                ob[:, at] = got
            stay(c, u).start()
            ticks(c, t + 2 + heads // GROUP)

        lax.fori_loop(0, half // UC, columns, None)

    pltpu.make_async_copy(x.at[pl.ds(0, R)], xn, x_s).start()
    for t in range(SLOTS):
        start_tile(jnp.int32(t), t)
    vb[:, HEAD:, :] = jnp.ones((heads, vb.shape[1] - HEAD, rows), BF16)

    for i in range(gain.shape[0]):
        wide_gain[:, i * HEAD : (i + 1) * HEAD] = jnp.broadcast_to(gain[i : i + 1, :].astype(F32), (8, HEAD))

    pltpu.make_async_copy(x.at[pl.ds(0, R)], xn, x_s).wait()
    lax.fori_loop(0, R // NR, lambda i, _: norm(i), None)

    def chunk(c, _):
        @pl.when(c > 0)
        def _():
            stay(c, 0).wait()
            share().wait_send()
            share().wait_recv()

        ticks(c, jnp.int32(0))
        project(c)
        attention(c)
        project_out(c)

    lax.fori_loop(0, chunks, chunk, None)

    stay(0, 0).wait()
    for u in range(2):
        away(0, u).wait_send()
    first = per * (chunks - 1) + late
    last = 2 * (pairs - 1) + max(FF, FM, FO, LM + 2 * LB + 2) + 1

    def rest(k, _):
        for h in range(2):
            tick(first + 2 * k + h, h)

    lax.fori_loop(0, (last + 1 - first + 1) // 2, rest, None)

    for p in range(pairs - OUT // 2, pairs):
        for h in range(2):
            sent(jnp.int32(p), h)

    def finish(c, _):
        rest_of = y.at[pl.ds(pl.multiple_of(c * R, R), R), pl.ds(pl.multiple_of((1 - core) * half, UC), half)]
        remote(rest_of, rest_of, fp_s.at[c], py_s.at[c], partner).wait_recv()
        few = y.at[pl.ds(0, R), pl.ds(0, half // 2)]

        @pl.when(mid)
        def _():
            remote(few, few, fo_s.at[c], y_s.at[0], outer).wait_send()
            remote(few, few, fp_s.at[c], py_s.at[c], partner).wait_send()

        @pl.when(end)
        def _():
            remote(rest_of, rest_of, fp_s.at[c], py_s.at[c], partner).wait_send()

    lax.fori_loop(0, chunks, finish, None)


def _whole(x, gain, cos, sin, wq, wk, wv, wo):
    rows, d = x.shape
    width = wq.shape[1]
    heads, half = width // HEAD, d // 2
    chunks = rows // R
    units = rows // UR * (half // UC)
    any_space, vmem = pl.BlockSpec(memory_space=pl.ANY), pl.BlockSpec(memory_space=pltpu.VMEM)
    dma = pltpu.SemaphoreType.DMA
    shape = jax.ShapeDtypeStruct
    flops = 2 * rows * d * width * 4 + 2 * rows * rows * width
    return pl.pallas_call(
        _kernel,
        out_shape=[shape((rows, d), BF16), shape((rows, half), F32), shape((rows, half), BF16), shape((rows, half), BF16), shape((rows, half), BF16)],
        in_specs=[any_space, vmem, vmem, vmem, any_space, any_space, any_space, any_space],
        out_specs=[any_space] * 5,
        scratch_shapes=[
            pltpu.VMEM((R, d), BF16),
            pltpu.VMEM((SLOTS, d, WT), BF16),
            pltpu.VMEM((R, WT), F32),
            pltpu.VMEM((heads, R, HEAD), BF16),
            pltpu.VMEM((heads, rows, HEAD), BF16),
            pltpu.VMEM((heads, HEAD + 16, rows), BF16),
            pltpu.VMEM((R, width), BF16),
            pltpu.VMEM((GROUP, 1, R), F32),
            pltpu.VMEM((GROUP, HEAD + 16, R), F32),
            pltpu.VMEM((8, d), F32),
            pltpu.VMEM((2, R, UC), BF16),
            pltpu.VMEM((R, UC), F32),
            pltpu.VMEM((2, UR, UC), F32),
            pltpu.VMEM((2, UR, UC), BF16),
            pltpu.VMEM((2, UR, UC), BF16),
            pltpu.VMEM((UR, UC), BF16),
            pltpu.VMEM((UR, UC), BF16),
            pltpu.VMEM((OUT, UR, UC), BF16),
            dma, dma((SLOTS,)), dma((2,)), dma,
            dma((chunks * (half // UC),)),
            dma((2,)), dma((2,)), dma((2,)), dma, dma,
            dma, dma, pltpu.SemaphoreType.REGULAR,
            dma((OUT, 4)),
            dma((units,)), dma((units // 2,)), dma((units,)),
            dma((chunks,)), dma((chunks,)), dma((chunks,)),
        ],
        compiler_params=pltpu.CompilerParams(collective_id=0, has_side_effects=True, vmem_limit_bytes=63 * 2**20),
        cost_estimate=pl.CostEstimate(flops=flops, transcendentals=rows * rows * heads, bytes_accessed=chunks * 4 * d * width * 2),
        name="layer",
    )(x, gain, cos, sin, wq, wk, wv, wo)[0]


def _turns(rows):
    half = HEAD // 2
    angle = np.arange(rows, dtype=np.float32)[:, None] * (float(THETA) ** (-np.arange(half) / half)).astype(np.float32)
    cos, sin = (f(angle.astype(np.float64)).astype(np.float32) for f in (np.cos, np.sin))
    return np.concatenate([cos, cos], -1), np.concatenate([-sin, sin], -1)


def solution(mesh):
    def step(x, gain, wq, wk, wv, wo):
        cos, sin = _turns(x.shape[0])
        return _whole(x, gain.reshape(-1, HEAD), jnp.asarray(cos), jnp.asarray(sin), wq, wk, wv, wo)

    tokens, columns = P("dp", None), P(None, "tp")
    return jax.shard_map(
        step,
        mesh=mesh,
        in_specs=(tokens, P(None), columns, columns, columns, P("tp", None)),
        out_specs=tokens,
        check_vma=False,
    )
```
